8 devices in a mesh: tp: 2 (over z, y), dp: 4 (over x, core).
Axes of the slice: x: 2, y: 2, z: 1, core: 2. Of those that a mesh axis runs over, the one named last changes fastest.
Arguments:
- a_mat: bfloat16 [5120, 32768], P(('dp', 'tp'))
- b_mat: bfloat16 [32768, 13824], P(('dp', 'tp'))
Outputs:
- output: bfloat16 [5120, 13824], P(('dp', 'tp'))
All inputs are finite; a program needn't handle non-finite values.
Results may differ from the reference program's by a relative error of at most 0.001.
Values are sent between devices in bfloat16 or wider.
A program may use at most 1 GiB of HBM per device.

```python
import jax
import jax.numpy as jnp

D_MODEL = 5120
D_FF = 13824
TOKENS_DEV = 4096
DEVICES = 8
TOKENS = TOKENS_DEV * DEVICES


def setup_inputs(seed: int = 0) -> dict:
    root_key = jax.random.key(seed)
    key_a, key_b = jax.random.split(root_key)
    acts_t = jax.random.normal(key_a, (D_MODEL, TOKENS), jnp.float32)
    grads = jax.random.normal(key_b, (TOKENS, D_FF), jnp.float32) * (TOKENS ** -0.5)
    return {"a_mat": acts_t.astype(jnp.bfloat16), "b_mat": grads.astype(jnp.bfloat16)}


def reference(a_mat, b_mat):
    prod = jnp.dot(a_mat, b_mat, preferred_element_type=jnp.float32)
    return prod.astype(jnp.bfloat16)
```

```python
import functools

import jax
import jax.numpy as jnp
from jax import lax
from jax.experimental import pallas as pl
from jax.experimental.pallas import tpu as pltpu
from jax.sharding import PartitionSpec as P

MESH = pl.DeviceIdType.MESH
HALF = 9
TILES = 2 * HALF
KSTEPS = 4
BCHUNKS = 4
WIDE = 256
OWN, FIRST, DIAG, SECOND = 0, 1, 2, 3


def _kernel(
    a_ref, b_ref, c_ref, a_got, b_got, part, first, fwd, last, summed,
    a_v, b_v, acc, add_v, out_v,
    a_send, a_recv, b_send, b_recv, p_send, p_recv, load_sem, b_sem, acc_sem, add_sem,
):
    rows = a_ref.shape[0]
    depth, cols = b_ref.shape
    tn = cols // TILES
    kc = depth // KSTEPS
    wide = min(WIDE, tn)

    dp, y = lax.axis_index("dp"), lax.axis_index("tp")
    x, core = dp // 2, dp % 2

    def device(dx, dc, dy):
        return {"dp": ((x + dx) % 2) * 2 + (core + dc) % 2, "tp": (y + dy) % 2}

    def a_cols(dx, dc, dy):
        block = ((x + dx) % 2) * 4 + ((core + dc) % 2) * 2 + (y + dy) % 2
        return pl.ds(pl.multiple_of(block * depth, depth), depth)

    barrier = pltpu.get_barrier_semaphore()
    for d in ((1, 0, 0), (0, 0, 1), (1, 0, 1), (0, 1, 0)):
        pl.semaphore_signal(barrier, inc=1, device_id=device(*d), device_id_type=MESH)
    pl.semaphore_wait(barrier, 4)

    bc = depth // BCHUNKS
    b_copies = [
        pltpu.make_async_remote_copy(
            src_ref=b_ref.at[pl.ds(j * bc, bc)],
            dst_ref=b_got.at[pl.ds(j * bc, bc)],
            send_sem=b_send.at[j],
            recv_sem=b_recv.at[j],
            device_id=device(0, 1, 0),
            device_id_type=MESH,
        )
        for j in range(BCHUNKS)
    ]
    a_copies = [
        [
            pltpu.make_async_remote_copy(
                src_ref=a_ref.at[:, a_cols(dx, dc, dy)],
                dst_ref=a_got.at[g, :, pl.ds(dc * depth, depth)],
                send_sem=a_send.at[g, dc],
                recv_sem=a_recv.at[g, dc],
                device_id=device(dx, 0, dy),
                device_id_type=MESH,
            )
            for dc in range(2)
        ]
        for g, (dx, dy) in enumerate(((1, 0), (0, 1), (1, 1)))
    ]
    for copy in b_copies:
        copy.start()
    for dc in range(2):
        a_copies[0][dc].start()
        a_copies[1][dc].start()
    for dc in range(2):
        a_copies[2][dc].start()

    own_loads = [
        pltpu.make_async_copy(
            a_ref.at[:, a_cols(0, dc, 0)], a_v.at[2, :, pl.ds(dc * depth, depth)], load_sem.at[dc]
        )
        for dc in range(2)
    ]
    for load in own_loads:
        load.start()
    for load in own_loads:
        load.wait()
    for copy in b_copies:
        copy.wait_recv()

    def place(i):
        return i % 2, i // 2 + HALF * (i % 2)

    def hop(par, dst, src, t, kind):
        return pltpu.make_async_remote_copy(
            src_ref=src,
            dst_ref=dst.at[t],
            send_sem=p_send.at[kind, t],
            recv_sem=p_recv.at[kind, t],
            device_id={"dp": ((x + 1 - par) % 2) * 2 + core, "tp": (y + par) % 2},
            device_id_type=MESH,
        )

    def b_loads(s):
        _, t = place(s // KSTEPS)
        k, slot = s % KSTEPS, s % 2
        at = (
            pl.ds(pl.multiple_of(k * kc, kc), kc),
            pl.ds(pl.multiple_of(t * tn, tn), tn),
        )
        return [
            pltpu.make_async_copy(ref.at[at], b_v.at[slot, h], b_sem.at[slot, h])
            for h, ref in enumerate((b_ref, b_got))
        ]

    def phase(which, a_slot, dst):
        def acc_out(i):
            _, t = place(i)
            return pltpu.make_async_copy(acc.at[i % 2], part.at[which, t], acc_sem.at[i % 2])

        def finish(i):
            acc_out(i).wait()
            if dst is not None:
                par, t = place(i)
                hop(par, dst, part.at[which, t], t, which - FIRST).start()

        for load in b_loads(0):
            load.start()

        def step(s, carry):
            i, k = s // KSTEPS, s % KSTEPS
            slot, into = s % 2, i % 2

            @pl.when(s + 1 < TILES * KSTEPS)
            def _():
                for load in b_loads(s + 1):
                    load.start()

            for load in b_loads(s):
                load.wait()
            a_at = a_slot(i % 2)
            near = pl.ds(pl.multiple_of(k * kc, kc), kc)
            far = pl.ds(pl.multiple_of(depth + k * kc, kc), kc)

            def piece(w, inner):
                at = pl.ds(pl.multiple_of(w * wide, wide), wide)
                dots = jnp.dot(
                    a_v[a_at, :, near], b_v[slot, 0, :, at], preferred_element_type=jnp.float32
                ) + jnp.dot(
                    a_v[a_at, :, far], b_v[slot, 1, :, at], preferred_element_type=jnp.float32
                )
                held = acc[into, :, at]
                acc[into, :, at] = jnp.where(k == 0, dots, held + dots)
                return inner

            lax.fori_loop(0, tn // wide, piece, 0)

            @pl.when(k == KSTEPS - 1)
            def _():
                acc_out(i).start()

                @pl.when(i > 0)
                def _():
                    finish(i - 1)

            return carry

        lax.fori_loop(0, TILES * KSTEPS, step, 0)
        finish(TILES - 1)

    def fetch(g, slot):
        for copy in a_copies[g]:
            copy.wait_recv()
        return pltpu.make_async_copy(a_got.at[g], a_v.at[slot], load_sem.at[slot])

    phase(OWN, lambda par: 2, None)
    loads = [fetch(0, 0), fetch(1, 1)]
    for load in loads:
        load.start()
    for load in loads:
        load.wait()
    phase(FIRST, lambda par: par, first)
    load = fetch(2, 2)
    load.start()
    load.wait()
    phase(DIAG, lambda par: 2, fwd)
    phase(SECOND, lambda par: 1 - par, None)

    def forward(i, carry):
        par, t = place(i)
        mine = pltpu.make_async_copy(part.at[SECOND, t], add_v.at[0], add_sem.at[0])
        mine.start()
        hop(par, fwd, part.at[DIAG, t], t, DIAG - FIRST).wait_recv()
        theirs = pltpu.make_async_copy(fwd.at[t], add_v.at[1], add_sem.at[1])
        theirs.start()
        mine.wait()
        theirs.wait()
        add_v[2] = add_v[0] + add_v[1]
        out = pltpu.make_async_copy(add_v.at[2], summed.at[t], add_sem.at[2])
        out.start()
        out.wait()
        hop(1 - par, last, summed.at[t], t, 2).start()
        return carry

    lax.fori_loop(0, TILES, forward, 0)

    def final(i, carry):
        par, t = place(i)
        own = pltpu.make_async_copy(part.at[OWN, t], add_v.at[0], add_sem.at[0])
        own.start()
        hop(par, first, part.at[FIRST, t], t, 0).wait_recv()
        near = pltpu.make_async_copy(first.at[t], add_v.at[1], add_sem.at[1])
        near.start()
        own.wait()
        near.wait()
        hop(1 - par, last, summed.at[t], t, 2).wait_recv()
        far = pltpu.make_async_copy(last.at[t], add_v.at[2], add_sem.at[2])
        far.start()
        far.wait()
        out_v[...] = (add_v[0] + add_v[1] + add_v[2]).astype(out_v.dtype)
        out = pltpu.make_async_copy(
            out_v, c_ref.at[:, pl.ds(pl.multiple_of(t * tn, tn), tn)], add_sem.at[3]
        )
        out.start()
        out.wait()
        return carry

    lax.fori_loop(0, TILES, final, 0)

    for copy in b_copies:
        copy.wait_send()
    for pair in a_copies:
        for copy in pair:
            copy.wait_send()

    def drain(i, carry):
        par, t = place(i)
        hop(par, first, part.at[FIRST, t], t, 0).wait_send()
        hop(par, fwd, part.at[DIAG, t], t, 1).wait_send()
        hop(1 - par, last, summed.at[t], t, 2).wait_send()
        return carry

    lax.fori_loop(0, TILES, drain, 0)


def solution(mesh):
    spec_rows = P(("dp", "tp"), None)

    def local_block(a_rows, b_rows):
        rows, inner = a_rows.shape
        depth, cols = b_rows.shape
        tn = cols // TILES
        f32, bf16 = jnp.float32, a_rows.dtype
        hbm = pl.BlockSpec(memory_space=pl.ANY)
        tiles = jax.ShapeDtypeStruct((TILES, rows, tn), f32)
        outs = pl.pallas_call(
            _kernel,
            out_shape=[
                jax.ShapeDtypeStruct((rows, cols), bf16),
                jax.ShapeDtypeStruct((3, rows, 2 * depth), bf16),
                jax.ShapeDtypeStruct((depth, cols), bf16),
                jax.ShapeDtypeStruct((4, TILES, rows, tn), f32),
                tiles,
                tiles,
                tiles,
                tiles,
            ],
            in_specs=[hbm] * 2,
            out_specs=[hbm] * 8,
            scratch_shapes=[
                pltpu.VMEM((3, rows, 2 * depth), bf16),
                pltpu.VMEM((2, 2, depth // KSTEPS, tn), bf16),
                pltpu.VMEM((2, rows, tn), f32),
                pltpu.VMEM((3, rows, tn), f32),
                pltpu.VMEM((rows, tn), bf16),
                pltpu.SemaphoreType.DMA((3, 2)),
                pltpu.SemaphoreType.DMA((3, 2)),
                pltpu.SemaphoreType.DMA((BCHUNKS,)),
                pltpu.SemaphoreType.DMA((BCHUNKS,)),
                pltpu.SemaphoreType.DMA((3, TILES)),
                pltpu.SemaphoreType.DMA((3, TILES)),
                pltpu.SemaphoreType.DMA((3,)),
                pltpu.SemaphoreType.DMA((2, 2)),
                pltpu.SemaphoreType.DMA((2,)),
                pltpu.SemaphoreType.DMA((4,)),
            ],
            compiler_params=pltpu.CompilerParams(
                collective_id=0, has_side_effects=True, vmem_limit_bytes=60 * 2**20
            ),
            cost_estimate=pl.CostEstimate(
                flops=2 * rows * inner * cols, bytes_accessed=2**30, transcendentals=0
            ),
        )(a_rows, b_rows)
        return outs[0]

    return jax.shard_map(local_block, mesh=mesh, in_specs=(spec_rows, spec_rows), out_specs=spec_rows, check_vma=False)
```

```python
import functools

import jax
import jax.numpy as jnp
from jax import lax
from jax.experimental import pallas as pl
from jax.experimental.pallas import tpu as pltpu
from jax.sharding import PartitionSpec as P

MESH = pl.DeviceIdType.MESH
HALF = 9
TILES = 2 * HALF
KSTEPS = 4
BCHUNKS = 4
WIDE = 256
OWN, FIRST, DIAG, SECOND = 0, 1, 2, 3


def _kernel(
    a_ref, b_ref, c_ref, a_got, b_got, part, first, fwd, last, summed,
    a_v, b_v, acc, add_v, last_v,
    a_send, a_recv, b_send, b_recv, p_send, p_recv, load_sem, b_sem, acc_sem, add_sem,
):
    rows = a_ref.shape[0]
    depth, cols = b_ref.shape
    tn = cols // TILES
    kc = depth // KSTEPS
    wide = min(WIDE, tn)

    dp, y = lax.axis_index("dp"), lax.axis_index("tp")
    x, core = dp // 2, dp % 2

    def device(dx, dc, dy):
        return {"dp": ((x + dx) % 2) * 2 + (core + dc) % 2, "tp": (y + dy) % 2}

    def a_cols(dx, dc, dy):
        block = ((x + dx) % 2) * 4 + ((core + dc) % 2) * 2 + (y + dy) % 2
        return pl.ds(pl.multiple_of(block * depth, depth), depth)

    barrier = pltpu.get_barrier_semaphore()
    for d in ((1, 0, 0), (0, 0, 1), (1, 0, 1), (0, 1, 0)):
        pl.semaphore_signal(barrier, inc=1, device_id=device(*d), device_id_type=MESH)
    pl.semaphore_wait(barrier, 4)

    bc = depth // BCHUNKS
    b_copies = [
        pltpu.make_async_remote_copy(
            src_ref=b_ref.at[pl.ds(j * bc, bc)],
            dst_ref=b_got.at[pl.ds(j * bc, bc)],
            send_sem=b_send.at[j],
            recv_sem=b_recv.at[j],
            device_id=device(0, 1, 0),
            device_id_type=MESH,
        )
        for j in range(BCHUNKS)
    ]
    a_copies = [
        [
            pltpu.make_async_remote_copy(
                src_ref=a_ref.at[:, a_cols(dx, dc, dy)],
                dst_ref=a_got.at[g, :, pl.ds(dc * depth, depth)],
                send_sem=a_send.at[g, dc],
                recv_sem=a_recv.at[g, dc],
                device_id=device(dx, 0, dy),
                device_id_type=MESH,
            )
            for dc in range(2)
        ]
        for g, (dx, dy) in enumerate(((1, 0), (0, 1), (1, 1)))
    ]
    for copy in b_copies:
        copy.start()
    for dc in range(2):
        a_copies[0][dc].start()
        a_copies[1][dc].start()
    for dc in range(2):
        a_copies[2][dc].start()

    own_loads = [
        pltpu.make_async_copy(
            a_ref.at[:, a_cols(0, dc, 0)], a_v.at[0, :, pl.ds(dc * depth, depth)], load_sem.at[dc]
        )
        for dc in range(2)
    ]
    for load in own_loads:
        load.start()
    for load in own_loads:
        load.wait()
    for copy in b_copies:
        copy.wait_recv()

    def place(i):
        return i % 2, i // 2 + HALF * (i % 2)

    def hop(par, dst, src, t, kind):
        return pltpu.make_async_remote_copy(
            src_ref=src,
            dst_ref=dst,
            send_sem=p_send.at[kind, t],
            recv_sem=p_recv.at[kind, t],
            device_id={"dp": ((x + 1 - par) % 2) * 2 + core, "tp": (y + par) % 2},
            device_id_type=MESH,
        )

    def b_loads(s):
        _, t = place(s // KSTEPS)
        k, slot = s % KSTEPS, s % 2
        at = (
            pl.ds(pl.multiple_of(k * kc, kc), kc),
            pl.ds(pl.multiple_of(t * tn, tn), tn),
        )
        return [
            pltpu.make_async_copy(ref.at[at], b_v.at[slot, h], b_sem.at[slot, h])
            for h, ref in enumerate((b_ref, b_got))
        ]

    def phase(which, a_slot, dst):
        def acc_out(i):
            _, t = place(i)
            return pltpu.make_async_copy(acc.at[i % 2], part.at[which, t], acc_sem.at[i % 2])

        def finish(i):
            acc_out(i).wait()
            if dst is not None:
                par, t = place(i)
                hop(par, dst.at[t], part.at[which, t], t, which - FIRST).start()

        for load in b_loads(0):
            load.start()

        def step(s, carry):
            i, k = s // KSTEPS, s % KSTEPS
            slot, into = s % 2, i % 2

            @pl.when(s + 1 < TILES * KSTEPS)
            def _():
                for load in b_loads(s + 1):
                    load.start()

            for load in b_loads(s):
                load.wait()
            a_at = a_slot(i % 2)
            near = pl.ds(pl.multiple_of(k * kc, kc), kc)
            far = pl.ds(pl.multiple_of(depth + k * kc, kc), kc)

            def piece(w, inner):
                at = pl.ds(pl.multiple_of(w * wide, wide), wide)
                dots = jnp.dot(
                    a_v[a_at, :, near], b_v[slot, 0, :, at], preferred_element_type=jnp.float32
                ) + jnp.dot(
                    a_v[a_at, :, far], b_v[slot, 1, :, at], preferred_element_type=jnp.float32
                )
                held = acc[into, :, at]
                acc[into, :, at] = jnp.where(k == 0, dots, held + dots)
                return inner

            lax.fori_loop(0, tn // wide, piece, 0)

            @pl.when(k == KSTEPS - 1)
            def _():
                acc_out(i).start()

                @pl.when(i > 0)
                def _():
                    finish(i - 1)

            return carry

        lax.fori_loop(0, TILES * KSTEPS, step, 0)
        finish(TILES - 1)

    def fetch(g, slot):
        for copy in a_copies[g]:
            copy.wait_recv()
        return pltpu.make_async_copy(a_got.at[g], a_v.at[slot], load_sem.at[slot])

    phase(OWN, lambda par: 0, None)
    loads = [fetch(0, 0), fetch(1, 1)]
    for load in loads:
        load.start()
    for load in loads:
        load.wait()
    phase(FIRST, lambda par: par, first)
    load = fetch(2, 0)
    load.start()
    load.wait()
    phase(DIAG, lambda par: 0, fwd)
    load = pltpu.make_async_copy(a_got.at[0], a_v.at[0], load_sem.at[0])
    load.start()
    load.wait()
    phase(SECOND, lambda par: 1 - par, None)

    def last_hop(i):
        par, t = place(i)
        dst = last.at[t] if not isinstance(i, int) or i < TILES - 2 else last_v.at[par]
        return hop(1 - par, dst, summed.at[t], t, 2)

    def forward(i, carry):
        par, t = place(i)
        mine = pltpu.make_async_copy(part.at[SECOND, t], add_v.at[0], add_sem.at[0])
        mine.start()
        hop(par, fwd.at[t], part.at[DIAG, t], t, 1).wait_recv()
        theirs = pltpu.make_async_copy(fwd.at[t], add_v.at[1], add_sem.at[1])
        theirs.start()
        mine.wait()
        theirs.wait()
        add_v[2] = add_v[0] + add_v[1]
        out = pltpu.make_async_copy(add_v.at[2], summed.at[t], add_sem.at[2])
        out.start()
        out.wait()
        last_hop(i).start()
        return carry

    lax.fori_loop(0, TILES - 2, forward, 0)
    for i in range(TILES - 2, TILES):
        forward(i, 0)

    def start_near(i, slot):
        par, t = place(i)
        own = pltpu.make_async_copy(part.at[OWN, t], add_v.at[slot], add_sem.at[slot])
        own.start()
        hop(par, first.at[t], part.at[FIRST, t], t, 0).wait_recv()
        near = pltpu.make_async_copy(first.at[t], add_v.at[slot + 1], add_sem.at[slot + 1])
        near.start()
        own.wait()
        near.wait()

    def columns(i):
        return pl.ds(pl.multiple_of(place(i)[1] * tn, tn), tn)

    def final(i, carry):
        start_near(i, 0)
        last_hop(i).wait_recv()
        far = pltpu.make_async_copy(last.at[place(i)[1]], add_v.at[2], add_sem.at[2])
        far.start()
        far.wait()
        c_ref[:, columns(i)] = (add_v[0] + add_v[1] + add_v[2]).astype(c_ref.dtype)
        return carry

    lax.fori_loop(0, TILES - 2, final, 0)
    for n, i in enumerate(range(TILES - 2, TILES)):
        start_near(i, n)
        add_v[n] = add_v[n] + add_v[n + 1]
    for n, i in enumerate(range(TILES - 2, TILES)):
        last_hop(i).wait_recv()
        c_ref[:, columns(i)] = (add_v[n] + last_v[n]).astype(c_ref.dtype)

    for copy in b_copies:
        copy.wait_send()
    for pair in a_copies:
        for copy in pair:
            copy.wait_send()

    def drain(i, carry):
        par, t = place(i)
        hop(par, first.at[t], part.at[FIRST, t], t, 0).wait_send()
        hop(par, fwd.at[t], part.at[DIAG, t], t, 1).wait_send()
        last_hop(i).wait_send()
        return carry

    lax.fori_loop(0, TILES - 2, drain, 0)
    for i in range(TILES - 2, TILES):
        drain(i, 0)


def solution(mesh):
    spec_rows = P(("dp", "tp"), None)

    def local_block(a_rows, b_rows):
        rows, inner = a_rows.shape
        depth, cols = b_rows.shape
        tn = cols // TILES
        f32, bf16 = jnp.float32, a_rows.dtype
        hbm = pl.BlockSpec(memory_space=pl.ANY)
        tiles = jax.ShapeDtypeStruct((TILES, rows, tn), f32)
        outs = pl.pallas_call(
            _kernel,
            out_shape=[
                pltpu.VMEM((rows, cols), bf16),
                jax.ShapeDtypeStruct((3, rows, 2 * depth), bf16),
                jax.ShapeDtypeStruct((depth, cols), bf16),
                jax.ShapeDtypeStruct((4, TILES, rows, tn), f32),
                tiles,
                tiles,
                tiles,
                tiles,
            ],
            in_specs=[hbm] * 2,
            out_specs=[pl.BlockSpec(memory_space=pltpu.VMEM)] + [hbm] * 7,
            scratch_shapes=[
                pltpu.VMEM((2, rows, 2 * depth), bf16),
                pltpu.VMEM((2, 2, depth // KSTEPS, tn), bf16),
                pltpu.VMEM((2, rows, tn), f32),
                pltpu.VMEM((3, rows, tn), f32),
                pltpu.VMEM((2, rows, tn), f32),
                pltpu.SemaphoreType.DMA((3, 2)),
                pltpu.SemaphoreType.DMA((3, 2)),
                pltpu.SemaphoreType.DMA((BCHUNKS,)),
                pltpu.SemaphoreType.DMA((BCHUNKS,)),
                pltpu.SemaphoreType.DMA((3, TILES)),
                pltpu.SemaphoreType.DMA((3, TILES)),
                pltpu.SemaphoreType.DMA((3,)),
                pltpu.SemaphoreType.DMA((2, 2)),
                pltpu.SemaphoreType.DMA((2,)),
                pltpu.SemaphoreType.DMA((3,)),
            ],
            compiler_params=pltpu.CompilerParams(
                collective_id=0, has_side_effects=True, vmem_limit_bytes=44 * 2**20
            ),
            cost_estimate=pl.CostEstimate(
                flops=2 * rows * inner * cols, bytes_accessed=2**30, transcendentals=0
            ),
        )(a_rows, b_rows)
        return outs[0]

    return jax.shard_map(local_block, mesh=mesh, in_specs=(spec_rows, spec_rows), out_specs=spec_rows, check_vma=False)
```

```python
import functools

import jax
import jax.numpy as jnp
from jax import lax
from jax.experimental import pallas as pl
from jax.experimental.pallas import tpu as pltpu
from jax.sharding import PartitionSpec as P

MESH = pl.DeviceIdType.MESH
HALF = 9
TILES = 2 * HALF
KSTEPS = 4
BCHUNKS = 4
WIDE = 256
BANDS = 4
OWN, FIRST, DIAG, SECOND = 0, 1, 2, 3


def _kernel(
    a_ref, b_ref, c_ref, near_v, last_v, a_got, b_got, part, first, fwd, last, summed,
    a_v, b_v, acc,
    a_send, a_recv, b_send, b_recv, p_send, p_recv, load_sem, b_sem, acc_sem, add_sem, across,
):
    rows = a_ref.shape[0]
    depth, cols = b_ref.shape
    tn = cols // TILES
    kc = depth // KSTEPS
    wide = min(WIDE, tn)

    dp, y = lax.axis_index("dp"), lax.axis_index("tp")
    x, core = dp // 2, dp % 2

    def device(dx, dc, dy):
        return {"dp": ((x + dx) % 2) * 2 + (core + dc) % 2, "tp": (y + dy) % 2}

    def a_cols(dx, dc, dy):
        block = ((x + dx) % 2) * 4 + ((core + dc) % 2) * 2 + (y + dy) % 2
        return pl.ds(pl.multiple_of(block * depth, depth), depth)

    barrier = pltpu.get_barrier_semaphore()
    for d in ((1, 0, 0), (0, 0, 1), (0, 1, 0)):
        pl.semaphore_signal(barrier, inc=1, device_id=device(*d), device_id_type=MESH)
    pl.semaphore_wait(barrier, 3)
    pl.semaphore_signal(across, inc=1, device_id=device(1, 0, 0), device_id_type=MESH)

    bc = depth // BCHUNKS
    b_copies = [
        pltpu.make_async_remote_copy(
            src_ref=b_ref.at[pl.ds(j * bc, bc)],
            dst_ref=b_got.at[pl.ds(j * bc, bc)],
            send_sem=b_send.at[j],
            recv_sem=b_recv.at[j],
            device_id=device(0, 1, 0),
            device_id_type=MESH,
        )
        for j in range(BCHUNKS)
    ]
    a_copies = [
        [
            pltpu.make_async_remote_copy(
                src_ref=a_ref.at[:, a_cols(dx, dc, dy)],
                dst_ref=a_got.at[g, :, pl.ds(dc * depth, depth)],
                send_sem=a_send.at[g, dc],
                recv_sem=a_recv.at[g, dc],
                device_id=device(dx, 0, dy),
                device_id_type=MESH,
            )
            for dc in range(2)
        ]
        for g, (dx, dy) in enumerate(((1, 0), (0, 1), (1, 1)))
    ]
    for copy in b_copies:
        copy.start()
    for dc in range(2):
        a_copies[0][dc].start()
        a_copies[1][dc].start()
    pl.semaphore_wait(across, 1)
    for dc in range(2):
        a_copies[2][dc].start()

    own_loads = [
        pltpu.make_async_copy(
            a_ref.at[:, a_cols(0, dc, 0)], a_v.at[0, :, pl.ds(dc * depth, depth)], load_sem.at[dc]
        )
        for dc in range(2)
    ]
    for load in own_loads:
        load.start()
    for load in own_loads:
        load.wait()
    for copy in b_copies:
        copy.wait_recv()

    def place(i):
        return i % 2, i // 2 + HALF * (i % 2)

    def hop(par, dst, src, t, kind):
        return pltpu.make_async_remote_copy(
            src_ref=src,
            dst_ref=dst,
            send_sem=p_send.at[kind, t],
            recv_sem=p_recv.at[kind, t],
            device_id={"dp": ((x + 1 - par) % 2) * 2 + core, "tp": (y + par) % 2},
            device_id_type=MESH,
        )

    def b_loads(s):
        _, t = place(s // KSTEPS)
        k, slot = s % KSTEPS, s % 2
        at = (
            pl.ds(pl.multiple_of(k * kc, kc), kc),
            pl.ds(pl.multiple_of(t * tn, tn), tn),
        )
        return [
            pltpu.make_async_copy(ref.at[at], b_v.at[slot, h], b_sem.at[slot, h])
            for h, ref in enumerate((b_ref, b_got))
        ]

    def phase(which, a_slot, dst):
        def acc_out(i):
            _, t = place(i)
            return pltpu.make_async_copy(acc.at[i % 2], part.at[which, t], acc_sem.at[i % 2])

        def finish(i):
            acc_out(i).wait()
            if dst is not None:
                par, t = place(i)
                hop(par, dst.at[t], part.at[which, t], t, which - FIRST).start()

        for load in b_loads(0):
            load.start()

        def step(s, carry):
            i, k = s // KSTEPS, s % KSTEPS
            slot, into = s % 2, i % 2

            @pl.when(s + 1 < TILES * KSTEPS)
            def _():
                for load in b_loads(s + 1):
                    load.start()

            for load in b_loads(s):
                load.wait()
            a_at = a_slot(i % 2)
            near = pl.ds(pl.multiple_of(k * kc, kc), kc)
            far = pl.ds(pl.multiple_of(depth + k * kc, kc), kc)

            def piece(w, inner):
                at = pl.ds(pl.multiple_of(w * wide, wide), wide)
                dots = jnp.dot(
                    a_v[a_at, :, near], b_v[slot, 0, :, at], preferred_element_type=jnp.float32
                ) + jnp.dot(
                    a_v[a_at, :, far], b_v[slot, 1, :, at], preferred_element_type=jnp.float32
                )
                held = acc[into, :, at]
                acc[into, :, at] = jnp.where(k == 0, dots, held + dots)
                return inner

            lax.fori_loop(0, tn // wide, piece, 0)

            @pl.when(k == KSTEPS - 1)
            def _():
                acc_out(i).start()

                @pl.when(i > 0)
                def _():
                    finish(i - 1)

            return carry

        lax.fori_loop(0, TILES * KSTEPS, step, 0)
        finish(TILES - 1)

    def fetch(g, slot):
        for copy in a_copies[g]:
            copy.wait_recv()
        return pltpu.make_async_copy(a_got.at[g], a_v.at[slot], load_sem.at[slot])

    phase(OWN, lambda par: 0, None)
    loads = [fetch(0, 0), fetch(1, 1)]
    for load in loads:
        load.start()
    for load in loads:
        load.wait()
    phase(FIRST, lambda par: par, first)
    load = fetch(2, 0)
    load.start()
    load.wait()
    phase(DIAG, lambda par: 0, fwd)
    load = pltpu.make_async_copy(a_got.at[0], a_v.at[0], load_sem.at[0])
    load.start()
    load.wait()
    phase(SECOND, lambda par: 1 - par, None)

    add_v = acc

    def last_hop(i):
        par, t = place(i)
        dst = last.at[t] if not isinstance(i, int) or i < TILES - 2 else last_v.at[par]
        return hop(1 - par, dst, summed.at[t], t, 2)

    def forward(i, carry):
        par, t = place(i)
        mine = pltpu.make_async_copy(part.at[SECOND, t], add_v.at[0], add_sem.at[0])
        mine.start()
        hop(par, fwd.at[t], part.at[DIAG, t], t, 1).wait_recv()
        theirs = pltpu.make_async_copy(fwd.at[t], add_v.at[1], add_sem.at[1])
        theirs.start()
        mine.wait()
        theirs.wait()
        add_v[0] = add_v[0] + add_v[1]
        out = pltpu.make_async_copy(add_v.at[0], summed.at[t], add_sem.at[0])
        out.start()
        out.wait()
        last_hop(i).start()
        return carry

    lax.fori_loop(0, TILES - 2, forward, 0)
    for i in range(TILES - 2, TILES):
        forward(i, 0)

    def near_terms(i):
        par, t = place(i)
        own = pltpu.make_async_copy(part.at[OWN, t], add_v.at[0], add_sem.at[0])
        own.start()
        hop(par, first.at[t], part.at[FIRST, t], t, 0).wait_recv()
        near = pltpu.make_async_copy(first.at[t], add_v.at[1], add_sem.at[1])
        near.start()
        own.wait()
        near.wait()
        return add_v[0] + add_v[1]

    def final(i, carry):
        _, t = place(i)
        add_v[0] = near_terms(i)
        last_hop(i).wait_recv()
        far = pltpu.make_async_copy(last.at[t], add_v.at[1], add_sem.at[1])
        far.start()
        far.wait()
        at = pl.ds(pl.multiple_of(t * tn, tn), tn)
        c_ref[:, at] = (add_v[0] + add_v[1]).astype(c_ref.dtype)
        return carry

    lax.fori_loop(0, TILES - 2, final, 0)
    for n, i in enumerate(range(TILES - 2, TILES)):
        near_v[n] = near_terms(i)
    for copy in b_copies:
        copy.wait_send()
    for pair in a_copies:
        for copy in pair:
            copy.wait_send()

    def drain(i, carry):
        par, t = place(i)
        hop(par, first.at[t], part.at[FIRST, t], t, 0).wait_send()
        hop(par, fwd.at[t], part.at[DIAG, t], t, 1).wait_send()
        last_hop(i).wait_send()
        return carry

    lax.fori_loop(0, TILES - 2, drain, 0)
    for i in range(TILES - 2, TILES):
        drain(i, 0)
        last_hop(i).wait_recv()


def _close(c_v, near_v, last_v, c_ref, out_v, sem, out_sem):
    rows, cols = c_ref.shape
    tn = cols // TILES
    band = rows // BANDS
    copies = []
    for h in range(2):
        at = pl.ds(h * HALF * tn, (HALF - 1) * tn)
        for r in range(BANDS):
            where = (pl.ds(r * band, band), at)
            copies.append(pltpu.make_async_copy(c_v.at[where], c_ref.at[where], sem.at[h, r]))
    for copy in copies:
        copy.start()
    for h in range(2):
        out_v[h] = (near_v[h] + last_v[h]).astype(out_v.dtype)
        at = pl.ds((h * HALF + HALF - 1) * tn, tn)
        copies.append(pltpu.make_async_copy(out_v.at[h], c_ref.at[:, at], out_sem.at[h]))
        copies[-1].start()
    for copy in copies:
        copy.wait()


def solution(mesh):
    spec_rows = P(("dp", "tp"), None)

    def local_block(a_rows, b_rows):
        rows, inner = a_rows.shape
        depth, cols = b_rows.shape
        tn = cols // TILES
        f32, bf16 = jnp.float32, a_rows.dtype
        hbm, vmem = pl.BlockSpec(memory_space=pl.ANY), pl.BlockSpec(memory_space=pltpu.VMEM)
        tiles = jax.ShapeDtypeStruct((TILES, rows, tn), f32)
        outs = pl.pallas_call(
            _kernel,
            out_shape=[
                pltpu.VMEM((rows, cols), bf16),
                pltpu.VMEM((2, rows, tn), f32),
                pltpu.VMEM((2, rows, tn), f32),
                jax.ShapeDtypeStruct((3, rows, 2 * depth), bf16),
                jax.ShapeDtypeStruct((depth, cols), bf16),
                jax.ShapeDtypeStruct((4, TILES, rows, tn), f32),
                tiles,
                tiles,
                tiles,
                tiles,
            ],
            in_specs=[hbm] * 2,
            out_specs=[vmem] * 3 + [hbm] * 7,
            scratch_shapes=[
                pltpu.VMEM((2, rows, 2 * depth), bf16),
                pltpu.VMEM((2, 2, depth // KSTEPS, tn), bf16),
                pltpu.VMEM((2, rows, tn), f32),
                pltpu.SemaphoreType.DMA((3, 2)),
                pltpu.SemaphoreType.DMA((3, 2)),
                pltpu.SemaphoreType.DMA((BCHUNKS,)),
                pltpu.SemaphoreType.DMA((BCHUNKS,)),
                pltpu.SemaphoreType.DMA((3, TILES)),
                pltpu.SemaphoreType.DMA((3, TILES)),
                pltpu.SemaphoreType.DMA((3,)),
                pltpu.SemaphoreType.DMA((2, 2)),
                pltpu.SemaphoreType.DMA((2,)),
                pltpu.SemaphoreType.DMA((2,)),
                pltpu.SemaphoreType.REGULAR,
            ],
            compiler_params=pltpu.CompilerParams(
                collective_id=0, has_side_effects=True, vmem_limit_bytes=37 * 2**20
            ),
            cost_estimate=pl.CostEstimate(
                flops=2 * rows * inner * cols, bytes_accessed=2**30, transcendentals=0
            ),
        )(a_rows, b_rows)
        held = [pltpu.with_memory_space_constraint(v, pltpu.VMEM) for v in outs[:3]]
        return pl.pallas_call(
            _close,
            out_shape=jax.ShapeDtypeStruct((rows, cols), bf16),
            in_specs=[vmem] * 3,
            out_specs=hbm,
            scratch_shapes=[
                pltpu.VMEM((2, rows, tn), bf16),
                pltpu.SemaphoreType.DMA((2, BANDS)),
                pltpu.SemaphoreType.DMA((2,)),
            ],
            compiler_params=pltpu.CompilerParams(vmem_limit_bytes=8 * 2**20),
        )(*held)

    return jax.shard_map(local_block, mesh=mesh, in_specs=(spec_rows, spec_rows), out_specs=spec_rows, check_vma=False)
```

```python
import functools

import jax
import jax.numpy as jnp
from jax import lax
from jax.experimental import pallas as pl
from jax.experimental.pallas import tpu as pltpu
from jax.sharding import PartitionSpec as P

MESH = pl.DeviceIdType.MESH
HALF = 9
TILES = 2 * HALF
KSTEPS = 4
BCHUNKS = 4
WIDE = 256
BANDS = 8
HEAD = 64
OWN, FIRST, DIAG, SECOND = 0, 1, 2, 3


def _kernel(
    a_ref, b_ref, c_ref, near_v, last_v, a_got, b_got, part, first, fwd, last, summed,
    a_v, b_v, acc,
    head_send, head_recv, head_sem, a_send, a_recv, b_send, b_recv, p_send, p_recv, load_sem, b_sem, acc_sem, add_sem, across,
):
    rows = a_ref.shape[0]
    depth, cols = b_ref.shape
    tn = cols // TILES
    kc = depth // KSTEPS
    wide = min(WIDE, tn)

    dp, y = lax.axis_index("dp"), lax.axis_index("tp")
    x, core = dp // 2, dp % 2

    def device(dx, dc, dy):
        return {"dp": ((x + dx) % 2) * 2 + (core + dc) % 2, "tp": (y + dy) % 2}

    def a_cols(dx, dc, dy):
        block = ((x + dx) % 2) * 4 + ((core + dc) % 2) * 2 + (y + dy) % 2
        return pl.ds(pl.multiple_of(block * depth, depth), depth)

    head = min(HEAD, rows // 2)
    sides = ((1, 0), (0, 1), (1, 1))
    staged = [a_v.at[1, pl.ds(g * head, head), pl.ds(0, depth)] for g in range(2)]
    head_loads = [
        pltpu.make_async_copy(
            a_ref.at[pl.ds(0, head), a_cols(sides[g][0], 0, sides[g][1])], staged[g], head_sem.at[g]
        )
        for g in range(2)
    ]
    for load in head_loads:
        load.start()

    barrier = pltpu.get_barrier_semaphore()
    for d in ((1, 0, 0), (0, 0, 1), (0, 1, 0)):
        pl.semaphore_signal(barrier, inc=1, device_id=device(*d), device_id_type=MESH)
    pl.semaphore_wait(barrier, 3)
    pl.semaphore_signal(across, inc=1, device_id=device(1, 0, 0), device_id_type=MESH)

    bc = depth // BCHUNKS
    b_copies = [
        pltpu.make_async_remote_copy(
            src_ref=b_ref.at[pl.ds(j * bc, bc)],
            dst_ref=b_got.at[pl.ds(j * bc, bc)],
            send_sem=b_send.at[j],
            recv_sem=b_recv.at[j],
            device_id=device(0, 1, 0),
            device_id_type=MESH,
        )
        for j in range(BCHUNKS)
    ]
    heads = [
        pltpu.make_async_remote_copy(
            src_ref=staged[g],
            dst_ref=a_got.at[g, pl.ds(0, head), pl.ds(0, depth)],
            send_sem=head_send.at[g],
            recv_sem=head_recv.at[g],
            device_id=device(sides[g][0], 0, sides[g][1]),
            device_id_type=MESH,
        )
        for g in range(2)
    ]

    def a_copy(g, dc):
        dx, dy = sides[g]
        top = head if g < 2 and dc == 0 else 0
        at = pl.ds(top, rows - top)
        return pltpu.make_async_remote_copy(
            src_ref=a_ref.at[at, a_cols(dx, dc, dy)],
            dst_ref=a_got.at[g, at, pl.ds(dc * depth, depth)],
            send_sem=a_send.at[g, dc],
            recv_sem=a_recv.at[g, dc],
            device_id=device(dx, 0, dy),
            device_id_type=MESH,
        )

    a_copies = [[a_copy(g, dc) for dc in range(2)] for g in range(3)]
    for load, copy in zip(head_loads, heads):
        load.wait()
        copy.start()
    for copy in b_copies:
        copy.start()
    for dc in range(2):
        a_copies[0][dc].start()
        a_copies[1][dc].start()
    pl.semaphore_wait(across, 1)
    for dc in range(2):
        a_copies[2][dc].start()

    own_loads = [
        pltpu.make_async_copy(
            a_ref.at[:, a_cols(0, dc, 0)], a_v.at[0, :, pl.ds(dc * depth, depth)], load_sem.at[dc]
        )
        for dc in range(2)
    ]
    for load in own_loads:
        load.start()
    for load in own_loads:
        load.wait()
    for copy in b_copies:
        copy.wait_recv()

    def place(i):
        return i % 2, i // 2 + HALF * (i % 2)

    def hop(par, dst, src, t, kind):
        return pltpu.make_async_remote_copy(
            src_ref=src,
            dst_ref=dst,
            send_sem=p_send.at[kind, t],
            recv_sem=p_recv.at[kind, t],
            device_id={"dp": ((x + 1 - par) % 2) * 2 + core, "tp": (y + par) % 2},
            device_id_type=MESH,
        )

    def b_loads(s):
        _, t = place(s // KSTEPS)
        k, slot = s % KSTEPS, s % 2
        at = (
            pl.ds(pl.multiple_of(k * kc, kc), kc),
            pl.ds(pl.multiple_of(t * tn, tn), tn),
        )
        return [
            pltpu.make_async_copy(ref.at[at], b_v.at[slot, h], b_sem.at[slot, h])
            for h, ref in enumerate((b_ref, b_got))
        ]

    def phase(which, a_slot, dst):
        def acc_out(i):
            _, t = place(i)
            return pltpu.make_async_copy(acc.at[i % 2], part.at[which, t], acc_sem.at[i % 2])

        def finish(i):
            acc_out(i).wait()
            if dst is not None:
                par, t = place(i)
                hop(par, dst.at[t], part.at[which, t], t, which - FIRST).start()

        for load in b_loads(0):
            load.start()

        def step(s, carry):
            i, k = s // KSTEPS, s % KSTEPS
            slot, into = s % 2, i % 2

            @pl.when(s + 1 < TILES * KSTEPS)
            def _():
                for load in b_loads(s + 1):
                    load.start()

            for load in b_loads(s):
                load.wait()
            a_at = a_slot(i % 2)
            near = pl.ds(pl.multiple_of(k * kc, kc), kc)
            far = pl.ds(pl.multiple_of(depth + k * kc, kc), kc)

            def piece(w, inner):
                at = pl.ds(pl.multiple_of(w * wide, wide), wide)
                dots = jnp.dot(
                    a_v[a_at, :, near], b_v[slot, 0, :, at], preferred_element_type=jnp.float32
                ) + jnp.dot(
                    a_v[a_at, :, far], b_v[slot, 1, :, at], preferred_element_type=jnp.float32
                )
                held = acc[into, :, at]
                acc[into, :, at] = jnp.where(k == 0, dots, held + dots)
                return inner

            lax.fori_loop(0, tn // wide, piece, 0)

            @pl.when(k == KSTEPS - 1)
            def _():
                acc_out(i).start()

                @pl.when(i > 0)
                def _():
                    finish(i - 1)

            return carry

        lax.fori_loop(0, TILES * KSTEPS, step, 0)
        finish(TILES - 1)

    def fetch(g, slot):
        for copy in a_copies[g]:
            copy.wait_recv()
        if g < 2:
            heads[g].wait_recv()
        return pltpu.make_async_copy(a_got.at[g], a_v.at[slot], load_sem.at[slot])

    phase(OWN, lambda par: 0, None)
    for copy in heads:
        copy.wait_send()
    loads = [fetch(0, 0), fetch(1, 1)]
    for load in loads:
        load.start()
    for load in loads:
        load.wait()
    phase(FIRST, lambda par: par, first)
    load = fetch(2, 0)
    load.start()
    load.wait()
    phase(DIAG, lambda par: 0, fwd)
    load = pltpu.make_async_copy(a_got.at[0], a_v.at[0], load_sem.at[0])
    load.start()
    load.wait()
    phase(SECOND, lambda par: 1 - par, None)

    add_v = acc

    def last_hop(i):
        par, t = place(i)
        dst = last.at[t] if not isinstance(i, int) or i < TILES - 2 else last_v.at[par]
        return hop(1 - par, dst, summed.at[t], t, 2)

    def forward(i, carry):
        par, t = place(i)
        mine = pltpu.make_async_copy(part.at[SECOND, t], add_v.at[0], add_sem.at[0])
        mine.start()
        hop(par, fwd.at[t], part.at[DIAG, t], t, 1).wait_recv()
        theirs = pltpu.make_async_copy(fwd.at[t], add_v.at[1], add_sem.at[1])
        theirs.start()
        mine.wait()
        theirs.wait()
        add_v[0] = add_v[0] + add_v[1]
        out = pltpu.make_async_copy(add_v.at[0], summed.at[t], add_sem.at[0])
        out.start()
        out.wait()
        last_hop(i).start()
        return carry

    lax.fori_loop(0, TILES - 2, forward, 0)
    for i in range(TILES - 2, TILES):
        forward(i, 0)

    def near_terms(i):
        par, t = place(i)
        own = pltpu.make_async_copy(part.at[OWN, t], add_v.at[0], add_sem.at[0])
        own.start()
        hop(par, first.at[t], part.at[FIRST, t], t, 0).wait_recv()
        near = pltpu.make_async_copy(first.at[t], add_v.at[1], add_sem.at[1])
        near.start()
        own.wait()
        near.wait()
        return add_v[0] + add_v[1]

    def final(i, carry):
        _, t = place(i)
        add_v[0] = near_terms(i)
        last_hop(i).wait_recv()
        far = pltpu.make_async_copy(last.at[t], add_v.at[1], add_sem.at[1])
        far.start()
        far.wait()
        at = pl.ds(pl.multiple_of(t * tn, tn), tn)
        c_ref[:, at] = (add_v[0] + add_v[1]).astype(c_ref.dtype)
        return carry

    lax.fori_loop(0, TILES - 2, final, 0)
    for n, i in enumerate(range(TILES - 2, TILES)):
        near_v[n] = near_terms(i)
    for copy in b_copies:
        copy.wait_send()
    for pair in a_copies:
        for copy in pair:
            copy.wait_send()

    def drain(i, carry):
        par, t = place(i)
        hop(par, first.at[t], part.at[FIRST, t], t, 0).wait_send()
        hop(par, fwd.at[t], part.at[DIAG, t], t, 1).wait_send()
        last_hop(i).wait_send()
        return carry

    lax.fori_loop(0, TILES - 2, drain, 0)
    for i in range(TILES - 2, TILES):
        drain(i, 0)
        last_hop(i).wait_recv()


def _close(c_v, near_v, last_v, c_ref, out_v, sem, out_sem):
    rows, cols = c_ref.shape
    tn = cols // TILES
    band = rows // BANDS
    copies = []
    for h in range(2):
        at = pl.ds(h * HALF * tn, (HALF - 1) * tn)
        for r in range(BANDS):
            where = (pl.ds(r * band, band), at)
            copies.append(pltpu.make_async_copy(c_v.at[where], c_ref.at[where], sem.at[h, r]))
    for copy in copies:
        copy.start()
    for h in range(2):
        out_v[h] = (near_v[h] + last_v[h]).astype(out_v.dtype)
        at = pl.ds((h * HALF + HALF - 1) * tn, tn)
        copies.append(pltpu.make_async_copy(out_v.at[h], c_ref.at[:, at], out_sem.at[h]))
        copies[-1].start()
    for copy in copies:
        copy.wait()


def solution(mesh):
    spec_rows = P(("dp", "tp"), None)

    def local_block(a_rows, b_rows):
        rows, inner = a_rows.shape
        depth, cols = b_rows.shape
        tn = cols // TILES
        f32, bf16 = jnp.float32, a_rows.dtype
        hbm, vmem = pl.BlockSpec(memory_space=pl.ANY), pl.BlockSpec(memory_space=pltpu.VMEM)
        tiles = jax.ShapeDtypeStruct((TILES, rows, tn), f32)
        outs = pl.pallas_call(
            _kernel,
            out_shape=[
                pltpu.VMEM((rows, cols), bf16),
                pltpu.VMEM((2, rows, tn), f32),
                pltpu.VMEM((2, rows, tn), f32),
                jax.ShapeDtypeStruct((3, rows, 2 * depth), bf16),
                jax.ShapeDtypeStruct((depth, cols), bf16),
                jax.ShapeDtypeStruct((4, TILES, rows, tn), f32),
                tiles,
                tiles,
                tiles,
                tiles,
            ],
            in_specs=[hbm] * 2,
            out_specs=[vmem] * 3 + [hbm] * 7,
            scratch_shapes=[
                pltpu.VMEM((2, rows, 2 * depth), bf16),
                pltpu.VMEM((2, 2, depth // KSTEPS, tn), bf16),
                pltpu.VMEM((2, rows, tn), f32),
                pltpu.SemaphoreType.DMA((2,)),
                pltpu.SemaphoreType.DMA((2,)),
                pltpu.SemaphoreType.DMA((2,)),
                pltpu.SemaphoreType.DMA((3, 2)),
                pltpu.SemaphoreType.DMA((3, 2)),
                pltpu.SemaphoreType.DMA((BCHUNKS,)),
                pltpu.SemaphoreType.DMA((BCHUNKS,)),
                pltpu.SemaphoreType.DMA((3, TILES)),
                pltpu.SemaphoreType.DMA((3, TILES)),
                pltpu.SemaphoreType.DMA((3,)),
                pltpu.SemaphoreType.DMA((2, 2)),
                pltpu.SemaphoreType.DMA((2,)),
                pltpu.SemaphoreType.DMA((2,)),
                pltpu.SemaphoreType.REGULAR,
            ],
            compiler_params=pltpu.CompilerParams(
                collective_id=0, has_side_effects=True, vmem_limit_bytes=37 * 2**20
            ),
            cost_estimate=pl.CostEstimate(
                flops=2 * rows * inner * cols, bytes_accessed=2**30, transcendentals=0
            ),
        )(a_rows, b_rows)
        held = [pltpu.with_memory_space_constraint(v, pltpu.VMEM) for v in outs[:3]]
        return pl.pallas_call(
            _close,
            out_shape=jax.ShapeDtypeStruct((rows, cols), bf16),
            in_specs=[vmem] * 3,
            out_specs=hbm,
            scratch_shapes=[
                pltpu.VMEM((2, rows, tn), bf16),
                pltpu.SemaphoreType.DMA((2, BANDS)),
                pltpu.SemaphoreType.DMA((2,)),
            ],
            compiler_params=pltpu.CompilerParams(vmem_limit_bytes=8 * 2**20),
        )(*held)

    return jax.shard_map(local_block, mesh=mesh, in_specs=(spec_rows, spec_rows), out_specs=spec_rows, check_vma=False)
```

```python
import functools

import jax
import jax.numpy as jnp
from jax import lax
from jax.experimental import pallas as pl
from jax.experimental.pallas import tpu as pltpu
from jax.sharding import PartitionSpec as P

MESH = pl.DeviceIdType.MESH
HALF = 9
TILES = 2 * HALF
KSTEPS = 4
BCHUNKS = 4
WIDE = 256
BANDS = 2
OWN, FIRST, DIAG, SECOND = 0, 1, 2, 3


def _kernel(
    a_ref, b_ref, c_ref, near_v, last_v, a_got, b_got, part, first, fwd, last, summed,
    a_v, b_v, acc,
    a_send, a_recv, b_send, b_recv, p_send, p_recv, load_sem, b_sem, acc_sem, add_sem, across,
):
    rows = a_ref.shape[0]
    depth, cols = b_ref.shape
    tn = cols // TILES
    kc = depth // KSTEPS
    wide = min(WIDE, tn)

    dp, y = lax.axis_index("dp"), lax.axis_index("tp")
    x, core = dp // 2, dp % 2

    def device(dx, dc, dy):
        return {"dp": ((x + dx) % 2) * 2 + (core + dc) % 2, "tp": (y + dy) % 2}

    def a_cols(dx, dc, dy):
        block = ((x + dx) % 2) * 4 + ((core + dc) % 2) * 2 + (y + dy) % 2
        return pl.ds(pl.multiple_of(block * depth, depth), depth)

    barrier = pltpu.get_barrier_semaphore()
    for d in ((1, 0, 0), (0, 0, 1), (0, 1, 0)):
        pl.semaphore_signal(barrier, inc=1, device_id=device(*d), device_id_type=MESH)
    pl.semaphore_wait(barrier, 3)
    pl.semaphore_signal(across, inc=1, device_id=device(1, 0, 0), device_id_type=MESH)

    bc = depth // BCHUNKS
    b_copies = [
        pltpu.make_async_remote_copy(
            src_ref=b_ref.at[pl.ds(j * bc, bc)],
            dst_ref=b_got.at[pl.ds(j * bc, bc)],
            send_sem=b_send.at[j],
            recv_sem=b_recv.at[j],
            device_id=device(0, 1, 0),
            device_id_type=MESH,
        )
        for j in range(BCHUNKS)
    ]
    a_copies = [
        [
            pltpu.make_async_remote_copy(
                src_ref=a_ref.at[:, a_cols(dx, dc, dy)],
                dst_ref=a_got.at[g, :, pl.ds(dc * depth, depth)],
                send_sem=a_send.at[g, dc],
                recv_sem=a_recv.at[g, dc],
                device_id=device(dx, 0, dy),
                device_id_type=MESH,
            )
            for dc in range(2)
        ]
        for g, (dx, dy) in enumerate(((1, 0), (0, 1), (1, 1)))
    ]
    for copy in b_copies:
        copy.start()
    for dc in range(2):
        a_copies[0][dc].start()
        a_copies[1][dc].start()
    pl.semaphore_wait(across, 1)
    for dc in range(2):
        a_copies[2][dc].start()

    own_loads = [
        pltpu.make_async_copy(
            a_ref.at[:, a_cols(0, dc, 0)], a_v.at[0, :, pl.ds(dc * depth, depth)], load_sem.at[dc]
        )
        for dc in range(2)
    ]
    for load in own_loads:
        load.start()
    for load in own_loads:
        load.wait()
    for copy in b_copies:
        copy.wait_recv()

    def place(i):
        return i % 2, i // 2 + HALF * (i % 2)

    def hop(par, dst, src, t, kind):
        return pltpu.make_async_remote_copy(
            src_ref=src,
            dst_ref=dst,
            send_sem=p_send.at[kind, t],
            recv_sem=p_recv.at[kind, t],
            device_id={"dp": ((x + 1 - par) % 2) * 2 + core, "tp": (y + par) % 2},
            device_id_type=MESH,
        )

    def b_loads(s):
        _, t = place(s // KSTEPS)
        k, slot = s % KSTEPS, s % 2
        at = (
            pl.ds(pl.multiple_of(k * kc, kc), kc),
            pl.ds(pl.multiple_of(t * tn, tn), tn),
        )
        return [
            pltpu.make_async_copy(ref.at[at], b_v.at[slot, h], b_sem.at[slot, h])
            for h, ref in enumerate((b_ref, b_got))
        ]

    def phase(which, a_slot, dst):
        def acc_out(i):
            _, t = place(i)
            return pltpu.make_async_copy(acc.at[i % 2], part.at[which, t], acc_sem.at[i % 2])

        def finish(i):
            acc_out(i).wait()
            if dst is not None:
                par, t = place(i)
                if which == FIRST:
                    @pl.when(i == 1)
                    def _():
                        for copy in a_copies[2]:
                            copy.wait_recv()

                hop(par, dst.at[t], part.at[which, t], t, which - FIRST).start()

        for load in b_loads(0):
            load.start()

        def step(s, carry):
            i, k = s // KSTEPS, s % KSTEPS
            slot, into = s % 2, i % 2

            @pl.when(s + 1 < TILES * KSTEPS)
            def _():
                for load in b_loads(s + 1):
                    load.start()

            for load in b_loads(s):
                load.wait()
            a_at = a_slot(i % 2)
            near = pl.ds(pl.multiple_of(k * kc, kc), kc)
            far = pl.ds(pl.multiple_of(depth + k * kc, kc), kc)

            def piece(w, inner):
                at = pl.ds(pl.multiple_of(w * wide, wide), wide)
                dots = jnp.dot(
                    a_v[a_at, :, near], b_v[slot, 0, :, at], preferred_element_type=jnp.float32
                ) + jnp.dot(
                    a_v[a_at, :, far], b_v[slot, 1, :, at], preferred_element_type=jnp.float32
                )
                held = acc[into, :, at]
                acc[into, :, at] = jnp.where(k == 0, dots, held + dots)
                return inner

            lax.fori_loop(0, tn // wide, piece, 0)

            @pl.when(k == KSTEPS - 1)
            def _():
                acc_out(i).start()

                @pl.when(i > 0)
                def _():
                    finish(i - 1)

            return carry

        lax.fori_loop(0, TILES * KSTEPS, step, 0)
        finish(TILES - 1)

    def fetch(g, slot):
        if g < 2:
            for copy in a_copies[g]:
                copy.wait_recv()
        return pltpu.make_async_copy(a_got.at[g], a_v.at[slot], load_sem.at[slot])

    phase(OWN, lambda par: 0, None)
    loads = [fetch(0, 0), fetch(1, 1)]
    for load in loads:
        load.start()
    for load in loads:
        load.wait()
    phase(FIRST, lambda par: par, first)
    load = fetch(2, 0)
    load.start()
    load.wait()
    phase(DIAG, lambda par: 0, fwd)
    load = pltpu.make_async_copy(a_got.at[0], a_v.at[0], load_sem.at[0])
    load.start()
    load.wait()
    phase(SECOND, lambda par: 1 - par, None)

    add_v = acc

    def last_hop(i):
        par, t = place(i)
        dst = last.at[t] if not isinstance(i, int) or i < TILES - 2 else last_v.at[par]
        return hop(1 - par, dst, summed.at[t], t, 2)

    def forward(i, carry):
        par, t = place(i)
        mine = pltpu.make_async_copy(part.at[SECOND, t], add_v.at[0], add_sem.at[0])
        mine.start()
        hop(par, fwd.at[t], part.at[DIAG, t], t, 1).wait_recv()
        theirs = pltpu.make_async_copy(fwd.at[t], add_v.at[1], add_sem.at[1])
        theirs.start()
        mine.wait()
        theirs.wait()
        add_v[0] = add_v[0] + add_v[1]
        out = pltpu.make_async_copy(add_v.at[0], summed.at[t], add_sem.at[0])
        out.start()
        out.wait()
        last_hop(i).start()
        return carry

    lax.fori_loop(0, TILES - 2, forward, 0)
    for i in range(TILES - 2, TILES):
        forward(i, 0)

    def near_terms(i):
        par, t = place(i)
        own = pltpu.make_async_copy(part.at[OWN, t], add_v.at[0], add_sem.at[0])
        own.start()
        hop(par, first.at[t], part.at[FIRST, t], t, 0).wait_recv()
        near = pltpu.make_async_copy(first.at[t], add_v.at[1], add_sem.at[1])
        near.start()
        own.wait()
        near.wait()
        return add_v[0] + add_v[1]

    def final(i, carry):
        _, t = place(i)
        add_v[0] = near_terms(i)
        last_hop(i).wait_recv()
        far = pltpu.make_async_copy(last.at[t], add_v.at[1], add_sem.at[1])
        far.start()
        far.wait()
        at = pl.ds(pl.multiple_of(t * tn, tn), tn)
        c_ref[:, at] = (add_v[0] + add_v[1]).astype(c_ref.dtype)
        return carry

    lax.fori_loop(0, TILES - 2, final, 0)
    for n, i in enumerate(range(TILES - 2, TILES)):
        near_v[n] = near_terms(i)
    for copy in b_copies:
        copy.wait_send()
    for pair in a_copies:
        for copy in pair:
            copy.wait_send()

    def drain(i, carry):
        par, t = place(i)
        hop(par, first.at[t], part.at[FIRST, t], t, 0).wait_send()
        hop(par, fwd.at[t], part.at[DIAG, t], t, 1).wait_send()
        last_hop(i).wait_send()
        return carry

    lax.fori_loop(0, TILES - 2, drain, 0)
    for i in range(TILES - 2, TILES):
        drain(i, 0)
        last_hop(i).wait_recv()


def _close(c_v, near_v, last_v, c_ref, out_v, sem, out_sem):
    rows, cols = c_ref.shape
    tn = cols // TILES
    band = rows // BANDS
    copies = []
    for h in range(2):
        at = pl.ds(h * HALF * tn, (HALF - 1) * tn)
        for r in range(BANDS):
            where = (pl.ds(r * band, band), at)
            copies.append(pltpu.make_async_copy(c_v.at[where], c_ref.at[where], sem.at[h, r]))
    for copy in copies:
        copy.start()
    for h in range(2):
        out_v[h] = (near_v[h] + last_v[h]).astype(out_v.dtype)
        at = pl.ds((h * HALF + HALF - 1) * tn, tn)
        copies.append(pltpu.make_async_copy(out_v.at[h], c_ref.at[:, at], out_sem.at[h]))
        copies[-1].start()
    for copy in copies:
        copy.wait()


def solution(mesh):
    spec_rows = P(("dp", "tp"), None)

    def local_block(a_rows, b_rows):
        rows, inner = a_rows.shape
        depth, cols = b_rows.shape
        tn = cols // TILES
        f32, bf16 = jnp.float32, a_rows.dtype
        hbm, vmem = pl.BlockSpec(memory_space=pl.ANY), pl.BlockSpec(memory_space=pltpu.VMEM)
        tiles = jax.ShapeDtypeStruct((TILES, rows, tn), f32)
        outs = pl.pallas_call(
            _kernel,
            out_shape=[
                pltpu.VMEM((rows, cols), bf16),
                pltpu.VMEM((2, rows, tn), f32),
                pltpu.VMEM((2, rows, tn), f32),
                jax.ShapeDtypeStruct((3, rows, 2 * depth), bf16),
                jax.ShapeDtypeStruct((depth, cols), bf16),
                jax.ShapeDtypeStruct((4, TILES, rows, tn), f32),
                tiles,
                tiles,
                tiles,
                tiles,
            ],
            in_specs=[hbm] * 2,
            out_specs=[vmem] * 3 + [hbm] * 7,
            scratch_shapes=[
                pltpu.VMEM((2, rows, 2 * depth), bf16),
                pltpu.VMEM((2, 2, depth // KSTEPS, tn), bf16),
                pltpu.VMEM((2, rows, tn), f32),
                pltpu.SemaphoreType.DMA((3, 2)),
                pltpu.SemaphoreType.DMA((3, 2)),
                pltpu.SemaphoreType.DMA((BCHUNKS,)),
                pltpu.SemaphoreType.DMA((BCHUNKS,)),
                pltpu.SemaphoreType.DMA((3, TILES)),
                pltpu.SemaphoreType.DMA((3, TILES)),
                pltpu.SemaphoreType.DMA((3,)),
                pltpu.SemaphoreType.DMA((2, 2)),
                pltpu.SemaphoreType.DMA((2,)),
                pltpu.SemaphoreType.DMA((2,)),
                pltpu.SemaphoreType.REGULAR,
            ],
            compiler_params=pltpu.CompilerParams(
                collective_id=0, has_side_effects=True, vmem_limit_bytes=37 * 2**20
            ),
            cost_estimate=pl.CostEstimate(
                flops=2 * rows * inner * cols, bytes_accessed=2**30, transcendentals=0
            ),
        )(a_rows, b_rows)
        held = [pltpu.with_memory_space_constraint(v, pltpu.VMEM) for v in outs[:3]]
        return pl.pallas_call(
            _close,
            out_shape=jax.ShapeDtypeStruct((rows, cols), bf16),
            in_specs=[vmem] * 3,
            out_specs=hbm,
            scratch_shapes=[
                pltpu.VMEM((2, rows, tn), bf16),
                pltpu.SemaphoreType.DMA((2, BANDS)),
                pltpu.SemaphoreType.DMA((2,)),
            ],
            compiler_params=pltpu.CompilerParams(vmem_limit_bytes=8 * 2**20),
        )(*held)

    return jax.shard_map(local_block, mesh=mesh, in_specs=(spec_rows, spec_rows), out_specs=spec_rows, check_vma=False)
```

```python
import functools

import jax
import jax.numpy as jnp
from jax import lax
from jax.experimental import pallas as pl
from jax.experimental.pallas import tpu as pltpu
from jax.sharding import PartitionSpec as P

MESH = pl.DeviceIdType.MESH
HALF = 9
TILES = 2 * HALF
KSTEPS = 4
BCHUNKS = 4
WIDE = 256
BANDS = 8
OWN, FIRST, DIAG, SECOND = 0, 1, 2, 3


def _kernel(
    a_ref, b_ref, c_ref, near_v, last_v, a_got, b_got, part, first, fwd, last, summed,
    a_v, b_v, acc,
    a_send, a_recv, b_send, b_recv, p_send, p_recv, load_sem, b_sem, acc_sem, add_sem, across,
):
    rows = a_ref.shape[0]
    depth, cols = b_ref.shape
    tn = cols // TILES
    kc = depth // KSTEPS
    wide = min(WIDE, tn)

    dp, y = lax.axis_index("dp"), lax.axis_index("tp")
    x, core = dp // 2, dp % 2

    def device(dx, dc, dy):
        return {"dp": ((x + dx) % 2) * 2 + (core + dc) % 2, "tp": (y + dy) % 2}

    def a_cols(dx, dc, dy):
        block = ((x + dx) % 2) * 4 + ((core + dc) % 2) * 2 + (y + dy) % 2
        return pl.ds(pl.multiple_of(block * depth, depth), depth)

    barrier = pltpu.get_barrier_semaphore()
    for d in ((1, 0, 0), (0, 0, 1), (0, 1, 0)):
        pl.semaphore_signal(barrier, inc=1, device_id=device(*d), device_id_type=MESH)
    pl.semaphore_wait(barrier, 3)
    pl.semaphore_signal(across, inc=1, device_id=device(1, 0, 0), device_id_type=MESH)

    bc = depth // BCHUNKS
    b_copies = [
        pltpu.make_async_remote_copy(
            src_ref=b_ref.at[pl.ds(j * bc, bc)],
            dst_ref=b_got.at[pl.ds(j * bc, bc)],
            send_sem=b_send.at[j],
            recv_sem=b_recv.at[j],
            device_id=device(0, 1, 0),
            device_id_type=MESH,
        )
        for j in range(BCHUNKS)
    ]
    a_copies = [
        [
            pltpu.make_async_remote_copy(
                src_ref=a_ref.at[:, a_cols(dx, dc, dy)],
                dst_ref=a_got.at[g, :, pl.ds(dc * depth, depth)],
                send_sem=a_send.at[g, dc],
                recv_sem=a_recv.at[g, dc],
                device_id=device(dx, 0, dy),
                device_id_type=MESH,
            )
            for dc in range(2)
        ]
        for g, (dx, dy) in enumerate(((1, 0), (0, 1), (1, 1)))
    ]
    for copy in b_copies:
        copy.start()
    for dc in range(2):
        a_copies[0][dc].start()
        a_copies[1][dc].start()
    pl.semaphore_wait(across, 1)
    for dc in range(2):
        a_copies[2][dc].start()

    own_loads = [
        pltpu.make_async_copy(
            a_ref.at[:, a_cols(0, dc, 0)], a_v.at[0, :, pl.ds(dc * depth, depth)], load_sem.at[dc]
        )
        for dc in range(2)
    ]
    for load in own_loads:
        load.start()
    for load in own_loads:
        load.wait()
    for copy in b_copies:
        copy.wait_recv()

    def place(i):
        return i % 2, i // 2 + HALF * (i % 2)

    def hop(par, dst, src, t, kind):
        return pltpu.make_async_remote_copy(
            src_ref=src,
            dst_ref=dst,
            send_sem=p_send.at[kind, t],
            recv_sem=p_recv.at[kind, t],
            device_id={"dp": ((x + 1 - par) % 2) * 2 + core, "tp": (y + par) % 2},
            device_id_type=MESH,
        )

    def b_loads(s):
        _, t = place(s // KSTEPS)
        k, slot = s % KSTEPS, s % 2
        at = (
            pl.ds(pl.multiple_of(k * kc, kc), kc),
            pl.ds(pl.multiple_of(t * tn, tn), tn),
        )
        return [
            pltpu.make_async_copy(ref.at[at], b_v.at[slot, h], b_sem.at[slot, h])
            for h, ref in enumerate((b_ref, b_got))
        ]

    def phase(which, a_slot, dst):
        def acc_out(i):
            _, t = place(i)
            return pltpu.make_async_copy(acc.at[i % 2], part.at[which, t], acc_sem.at[i % 2])

        def finish(i):
            acc_out(i).wait()
            if dst is not None:
                par, t = place(i)
                hop(par, dst.at[t], part.at[which, t], t, which - FIRST).start()

        for load in b_loads(0):
            load.start()

        def step(s, carry):
            i, k = s // KSTEPS, s % KSTEPS
            slot, into = s % 2, i % 2

            @pl.when(s + 1 < TILES * KSTEPS)
            def _():
                for load in b_loads(s + 1):
                    load.start()

            for load in b_loads(s):
                load.wait()
            a_at = a_slot(i % 2)
            near = pl.ds(pl.multiple_of(k * kc, kc), kc)
            far = pl.ds(pl.multiple_of(depth + k * kc, kc), kc)

            def piece(w, inner):
                at = pl.ds(pl.multiple_of(w * wide, wide), wide)
                dots = jnp.dot(
                    a_v[a_at, :, near], b_v[slot, 0, :, at], preferred_element_type=jnp.float32
                ) + jnp.dot(
                    a_v[a_at, :, far], b_v[slot, 1, :, at], preferred_element_type=jnp.float32
                )
                held = acc[into, :, at]
                acc[into, :, at] = jnp.where(k == 0, dots, held + dots)
                return inner

            lax.fori_loop(0, tn // wide, piece, 0)

            @pl.when(k == KSTEPS - 1)
            def _():
                acc_out(i).start()

                @pl.when(i > 0)
                def _():
                    finish(i - 1)

            return carry

        lax.fori_loop(0, TILES * KSTEPS, step, 0)
        finish(TILES - 1)

    def fetch(g, slot):
        for copy in a_copies[g]:
            copy.wait_recv()
        return pltpu.make_async_copy(a_got.at[g], a_v.at[slot], load_sem.at[slot])

    phase(OWN, lambda par: 0, None)
    loads = [fetch(0, 0), fetch(1, 1)]
    for load in loads:
        load.start()
    for load in loads:
        load.wait()
    phase(FIRST, lambda par: par, first)
    load = fetch(2, 0)
    load.start()
    load.wait()
    phase(DIAG, lambda par: 0, fwd)
    load = pltpu.make_async_copy(a_got.at[0], a_v.at[0], load_sem.at[0])
    load.start()
    load.wait()
    phase(SECOND, lambda par: 1 - par, None)

    add_v = acc

    def last_hop(i):
        par, t = place(i)
        dst = last.at[t] if not isinstance(i, int) or i < TILES - 2 else last_v.at[par]
        return hop(1 - par, dst, summed.at[t], t, 2)

    def forward(i, carry):
        par, t = place(i)
        mine = pltpu.make_async_copy(part.at[SECOND, t], add_v.at[0], add_sem.at[0])
        mine.start()
        hop(par, fwd.at[t], part.at[DIAG, t], t, 1).wait_recv()
        theirs = pltpu.make_async_copy(fwd.at[t], add_v.at[1], add_sem.at[1])
        theirs.start()
        mine.wait()
        theirs.wait()
        add_v[0] = add_v[0] + add_v[1]
        out = pltpu.make_async_copy(add_v.at[0], summed.at[t], add_sem.at[0])
        out.start()
        out.wait()
        last_hop(i).start()
        return carry

    lax.fori_loop(0, TILES - 2, forward, 0)
    for i in range(TILES - 2, TILES):
        forward(i, 0)

    def near_terms(i):
        par, t = place(i)
        own = pltpu.make_async_copy(part.at[OWN, t], add_v.at[0], add_sem.at[0])
        own.start()
        hop(par, first.at[t], part.at[FIRST, t], t, 0).wait_recv()
        near = pltpu.make_async_copy(first.at[t], add_v.at[1], add_sem.at[1])
        near.start()
        own.wait()
        near.wait()
        return add_v[0] + add_v[1]

    def final(i, carry):
        _, t = place(i)
        add_v[0] = near_terms(i)
        last_hop(i).wait_recv()
        far = pltpu.make_async_copy(last.at[t], add_v.at[1], add_sem.at[1])
        far.start()
        far.wait()
        at = pl.ds(pl.multiple_of(t * tn, tn), tn)
        c_ref[:, at] = (add_v[0] + add_v[1]).astype(c_ref.dtype)
        return carry

    lax.fori_loop(0, TILES - 2, final, 0)
    for n, i in enumerate(range(TILES - 2, TILES)):
        near_v[n] = near_terms(i)
    for copy in b_copies:
        copy.wait_send()
    for pair in a_copies:
        for copy in pair:
            copy.wait_send()

    def drain(i, carry):
        par, t = place(i)
        hop(par, first.at[t], part.at[FIRST, t], t, 0).wait_send()
        hop(par, fwd.at[t], part.at[DIAG, t], t, 1).wait_send()
        last_hop(i).wait_send()
        return carry

    lax.fori_loop(0, TILES - 2, drain, 0)
    for i in range(TILES - 2, TILES):
        drain(i, 0)
        last_hop(i).wait_recv()


def _close(c_in, near_v, last_v, c_v, c_ref, sem):
    del c_in
    rows, cols = c_ref.shape
    tn = cols // TILES
    band = rows // BANDS
    copies = []
    for r in range(BANDS):
        at = pl.ds(r * band, band)
        for h in range(2):
            tile = pl.ds((h * HALF + HALF - 1) * tn, tn)
            c_v[at, tile] = (near_v[h, at] + last_v[h, at]).astype(c_v.dtype)
        if r:
            copies[-1].start()
        copies.append(pltpu.make_async_copy(c_v.at[at], c_ref.at[at], sem.at[r]))
    copies[-1].start()
    for copy in copies:
        copy.wait()


def solution(mesh):
    spec_rows = P(("dp", "tp"), None)

    def local_block(a_rows, b_rows):
        rows, inner = a_rows.shape
        depth, cols = b_rows.shape
        tn = cols // TILES
        f32, bf16 = jnp.float32, a_rows.dtype
        hbm, vmem = pl.BlockSpec(memory_space=pl.ANY), pl.BlockSpec(memory_space=pltpu.VMEM)
        tiles = jax.ShapeDtypeStruct((TILES, rows, tn), f32)
        outs = pl.pallas_call(
            _kernel,
            out_shape=[
                pltpu.VMEM((rows, cols), bf16),
                pltpu.VMEM((2, rows, tn), f32),
                pltpu.VMEM((2, rows, tn), f32),
                jax.ShapeDtypeStruct((3, rows, 2 * depth), bf16),
                jax.ShapeDtypeStruct((depth, cols), bf16),
                jax.ShapeDtypeStruct((4, TILES, rows, tn), f32),
                tiles,
                tiles,
                tiles,
                tiles,
            ],
            in_specs=[hbm] * 2,
            out_specs=[vmem] * 3 + [hbm] * 7,
            scratch_shapes=[
                pltpu.VMEM((2, rows, 2 * depth), bf16),
                pltpu.VMEM((2, 2, depth // KSTEPS, tn), bf16),
                pltpu.VMEM((2, rows, tn), f32),
                pltpu.SemaphoreType.DMA((3, 2)),
                pltpu.SemaphoreType.DMA((3, 2)),
                pltpu.SemaphoreType.DMA((BCHUNKS,)),
                pltpu.SemaphoreType.DMA((BCHUNKS,)),
                pltpu.SemaphoreType.DMA((3, TILES)),
                pltpu.SemaphoreType.DMA((3, TILES)),
                pltpu.SemaphoreType.DMA((3,)),
                pltpu.SemaphoreType.DMA((2, 2)),
                pltpu.SemaphoreType.DMA((2,)),
                pltpu.SemaphoreType.DMA((2,)),
                pltpu.SemaphoreType.REGULAR,
            ],
            compiler_params=pltpu.CompilerParams(
                collective_id=0, has_side_effects=True, vmem_limit_bytes=37 * 2**20
            ),
            cost_estimate=pl.CostEstimate(
                flops=2 * rows * inner * cols, bytes_accessed=2**30, transcendentals=0
            ),
        )(a_rows, b_rows)
        held = [pltpu.with_memory_space_constraint(v, pltpu.VMEM) for v in outs[:3]]
        return pl.pallas_call(
            _close,
            out_shape=[pltpu.VMEM((rows, cols), bf16), jax.ShapeDtypeStruct((rows, cols), bf16)],
            in_specs=[vmem] * 3,
            out_specs=[vmem, hbm],
            input_output_aliases={0: 0},
            scratch_shapes=[pltpu.SemaphoreType.DMA((BANDS,))],
            compiler_params=pltpu.CompilerParams(vmem_limit_bytes=8 * 2**20),
        )(*held)[1]

    return jax.shard_map(local_block, mesh=mesh, in_specs=(spec_rows, spec_rows), out_specs=spec_rows, check_vma=False)
```

```python
import functools

import jax
import jax.numpy as jnp
from jax import lax
from jax.experimental import pallas as pl
from jax.experimental.pallas import tpu as pltpu
from jax.sharding import PartitionSpec as P

MESH = pl.DeviceIdType.MESH
HALF = 9
TILES = 2 * HALF
KSTEPS = 4
BCHUNKS = 4
WIDE = 256
BANDS = 4
OWN, FIRST, DIAG, SECOND = 0, 1, 2, 3


def _kernel(
    a_ref, b_ref, c_ref, near_v, last_v, a_got, b_got, part, first, fwd, last, summed,
    a_v, b_v, acc,
    a_send, a_recv, b_send, b_recv, p_send, p_recv, load_sem, b_sem, acc_sem, add_sem, across,
):
    rows = a_ref.shape[0]
    depth, cols = b_ref.shape
    tn = cols // TILES
    kc = depth // KSTEPS
    wide = min(WIDE, tn)

    dp, y = lax.axis_index("dp"), lax.axis_index("tp")
    x, core = dp // 2, dp % 2

    def device(dx, dc, dy):
        return {"dp": ((x + dx) % 2) * 2 + (core + dc) % 2, "tp": (y + dy) % 2}

    def a_cols(dx, dc, dy):
        block = ((x + dx) % 2) * 4 + ((core + dc) % 2) * 2 + (y + dy) % 2
        return pl.ds(pl.multiple_of(block * depth, depth), depth)

    barrier = pltpu.get_barrier_semaphore()
    for d in ((1, 0, 0), (0, 0, 1), (0, 1, 0)):
        pl.semaphore_signal(barrier, inc=1, device_id=device(*d), device_id_type=MESH)
    pl.semaphore_wait(barrier, 3)
    pl.semaphore_signal(across, inc=1, device_id=device(1, 0, 0), device_id_type=MESH)

    bc = depth // BCHUNKS
    b_copies = [
        pltpu.make_async_remote_copy(
            src_ref=b_ref.at[pl.ds(j * bc, bc)],
            dst_ref=b_got.at[pl.ds(j * bc, bc)],
            send_sem=b_send.at[j],
            recv_sem=b_recv.at[j],
            device_id=device(0, 1, 0),
            device_id_type=MESH,
        )
        for j in range(BCHUNKS)
    ]
    a_copies = [
        [
            pltpu.make_async_remote_copy(
                src_ref=a_ref.at[:, a_cols(dx, dc, dy)],
                dst_ref=a_got.at[g, :, pl.ds(dc * depth, depth)],
                send_sem=a_send.at[g, dc],
                recv_sem=a_recv.at[g, dc],
                device_id=device(dx, 0, dy),
                device_id_type=MESH,
            )
            for dc in range(2)
        ]
        for g, (dx, dy) in enumerate(((1, 0), (0, 1), (1, 1)))
    ]
    for g in range(2):
        a_copies[g][0].start()
    for copy in b_copies:
        copy.start()
    for g in range(2):
        a_copies[g][1].start()
    pl.semaphore_wait(across, 1)
    for dc in range(2):
        a_copies[2][dc].start()

    own_loads = [
        pltpu.make_async_copy(
            a_ref.at[:, a_cols(0, dc, 0)], a_v.at[0, :, pl.ds(dc * depth, depth)], load_sem.at[dc]
        )
        for dc in range(2)
    ]
    for load in own_loads:
        load.start()
    for load in own_loads:
        load.wait()
    for copy in b_copies:
        copy.wait_recv()

    def place(i):
        return i % 2, i // 2 + HALF * (i % 2)

    def hop(par, dst, src, t, kind):
        return pltpu.make_async_remote_copy(
            src_ref=src,
            dst_ref=dst,
            send_sem=p_send.at[kind, t],
            recv_sem=p_recv.at[kind, t],
            device_id={"dp": ((x + 1 - par) % 2) * 2 + core, "tp": (y + par) % 2},
            device_id_type=MESH,
        )

    def b_loads(s):
        _, t = place(s // KSTEPS)
        k, slot = s % KSTEPS, s % 2
        at = (
            pl.ds(pl.multiple_of(k * kc, kc), kc),
            pl.ds(pl.multiple_of(t * tn, tn), tn),
        )
        return [
            pltpu.make_async_copy(ref.at[at], b_v.at[slot, h], b_sem.at[slot, h])
            for h, ref in enumerate((b_ref, b_got))
        ]

    def phase(which, a_slot, dst):
        def acc_out(i):
            _, t = place(i)
            return pltpu.make_async_copy(acc.at[i % 2], part.at[which, t], acc_sem.at[i % 2])

        def finish(i):
            acc_out(i).wait()
            if dst is not None:
                par, t = place(i)
                hop(par, dst.at[t], part.at[which, t], t, which - FIRST).start()

        for load in b_loads(0):
            load.start()

        def step(s, carry):
            i, k = s // KSTEPS, s % KSTEPS
            slot, into = s % 2, i % 2

            @pl.when(s + 1 < TILES * KSTEPS)
            def _():
                for load in b_loads(s + 1):
                    load.start()

            for load in b_loads(s):
                load.wait()
            a_at = a_slot(i % 2)
            near = pl.ds(pl.multiple_of(k * kc, kc), kc)
            far = pl.ds(pl.multiple_of(depth + k * kc, kc), kc)

            def piece(w, inner):
                at = pl.ds(pl.multiple_of(w * wide, wide), wide)
                dots = jnp.dot(
                    a_v[a_at, :, near], b_v[slot, 0, :, at], preferred_element_type=jnp.float32
                ) + jnp.dot(
                    a_v[a_at, :, far], b_v[slot, 1, :, at], preferred_element_type=jnp.float32
                )
                held = acc[into, :, at]
                acc[into, :, at] = jnp.where(k == 0, dots, held + dots)
                return inner

            lax.fori_loop(0, tn // wide, piece, 0)

            @pl.when(k == KSTEPS - 1)
            def _():
                acc_out(i).start()

                @pl.when(i > 0)
                def _():
                    finish(i - 1)

            return carry

        lax.fori_loop(0, TILES * KSTEPS, step, 0)
        finish(TILES - 1)

    def fetch(g, slot):
        for copy in a_copies[g]:
            copy.wait_recv()
        return pltpu.make_async_copy(a_got.at[g], a_v.at[slot], load_sem.at[slot])

    phase(OWN, lambda par: 0, None)
    loads = [fetch(0, 0), fetch(1, 1)]
    for load in loads:
        load.start()
    for load in loads:
        load.wait()
    phase(FIRST, lambda par: par, first)
    load = fetch(2, 0)
    load.start()
    load.wait()
    phase(DIAG, lambda par: 0, fwd)
    load = pltpu.make_async_copy(a_got.at[0], a_v.at[0], load_sem.at[0])
    load.start()
    load.wait()
    phase(SECOND, lambda par: 1 - par, None)

    add_v = acc

    def last_hop(i):
        par, t = place(i)
        dst = last.at[t] if not isinstance(i, int) or i < TILES - 2 else last_v.at[par]
        return hop(1 - par, dst, summed.at[t], t, 2)

    def forward(i, carry):
        par, t = place(i)
        mine = pltpu.make_async_copy(part.at[SECOND, t], add_v.at[0], add_sem.at[0])
        mine.start()
        hop(par, fwd.at[t], part.at[DIAG, t], t, 1).wait_recv()
        theirs = pltpu.make_async_copy(fwd.at[t], add_v.at[1], add_sem.at[1])
        theirs.start()
        mine.wait()
        theirs.wait()
        add_v[0] = add_v[0] + add_v[1]
        out = pltpu.make_async_copy(add_v.at[0], summed.at[t], add_sem.at[0])
        out.start()
        out.wait()
        last_hop(i).start()
        return carry

    lax.fori_loop(0, TILES - 2, forward, 0)
    for i in range(TILES - 2, TILES):
        forward(i, 0)

    def near_terms(i):
        par, t = place(i)
        own = pltpu.make_async_copy(part.at[OWN, t], add_v.at[0], add_sem.at[0])
        own.start()
        hop(par, first.at[t], part.at[FIRST, t], t, 0).wait_recv()
        near = pltpu.make_async_copy(first.at[t], add_v.at[1], add_sem.at[1])
        near.start()
        own.wait()
        near.wait()
        return add_v[0] + add_v[1]

    def final(i, carry):
        _, t = place(i)
        add_v[0] = near_terms(i)
        last_hop(i).wait_recv()
        far = pltpu.make_async_copy(last.at[t], add_v.at[1], add_sem.at[1])
        far.start()
        far.wait()
        at = pl.ds(pl.multiple_of(t * tn, tn), tn)
        c_ref[:, at] = (add_v[0] + add_v[1]).astype(c_ref.dtype)
        return carry

    lax.fori_loop(0, TILES - 2, final, 0)
    for n, i in enumerate(range(TILES - 2, TILES)):
        near_v[n] = near_terms(i)
    for copy in b_copies:
        copy.wait_send()
    for pair in a_copies:
        for copy in pair:
            copy.wait_send()

    def drain(i, carry):
        par, t = place(i)
        hop(par, first.at[t], part.at[FIRST, t], t, 0).wait_send()
        hop(par, fwd.at[t], part.at[DIAG, t], t, 1).wait_send()
        last_hop(i).wait_send()
        return carry

    lax.fori_loop(0, TILES - 2, drain, 0)
    for i in range(TILES - 2, TILES):
        drain(i, 0)
        last_hop(i).wait_recv()


def _close(c_v, near_v, last_v, c_ref, out_v, sem, out_sem):
    rows, cols = c_ref.shape
    tn = cols // TILES
    band = rows // BANDS
    copies = []
    for h in range(2):
        at = pl.ds(h * HALF * tn, (HALF - 1) * tn)
        for r in range(BANDS):
            where = (pl.ds(r * band, band), at)
            copies.append(pltpu.make_async_copy(c_v.at[where], c_ref.at[where], sem.at[h, r]))
    for copy in copies:
        copy.start()
    for h in range(2):
        out_v[h] = (near_v[h] + last_v[h]).astype(out_v.dtype)
        at = pl.ds((h * HALF + HALF - 1) * tn, tn)
        copies.append(pltpu.make_async_copy(out_v.at[h], c_ref.at[:, at], out_sem.at[h]))
        copies[-1].start()
    for copy in copies:
        copy.wait()


def solution(mesh):
    spec_rows = P(("dp", "tp"), None)

    def local_block(a_rows, b_rows):
        rows, inner = a_rows.shape
        depth, cols = b_rows.shape
        tn = cols // TILES
        f32, bf16 = jnp.float32, a_rows.dtype
        hbm, vmem = pl.BlockSpec(memory_space=pl.ANY), pl.BlockSpec(memory_space=pltpu.VMEM)
        tiles = jax.ShapeDtypeStruct((TILES, rows, tn), f32)
        outs = pl.pallas_call(
            _kernel,
            out_shape=[
                pltpu.VMEM((rows, cols), bf16),
                pltpu.VMEM((2, rows, tn), f32),
                pltpu.VMEM((2, rows, tn), f32),
                jax.ShapeDtypeStruct((3, rows, 2 * depth), bf16),
                jax.ShapeDtypeStruct((depth, cols), bf16),
                jax.ShapeDtypeStruct((4, TILES, rows, tn), f32),
                tiles,
                tiles,
                tiles,
                tiles,
            ],
            in_specs=[hbm] * 2,
            out_specs=[vmem] * 3 + [hbm] * 7,
            scratch_shapes=[
                pltpu.VMEM((2, rows, 2 * depth), bf16),
                pltpu.VMEM((2, 2, depth // KSTEPS, tn), bf16),
                pltpu.VMEM((2, rows, tn), f32),
                pltpu.SemaphoreType.DMA((3, 2)),
                pltpu.SemaphoreType.DMA((3, 2)),
                pltpu.SemaphoreType.DMA((BCHUNKS,)),
                pltpu.SemaphoreType.DMA((BCHUNKS,)),
                pltpu.SemaphoreType.DMA((3, TILES)),
                pltpu.SemaphoreType.DMA((3, TILES)),
                pltpu.SemaphoreType.DMA((3,)),
                pltpu.SemaphoreType.DMA((2, 2)),
                pltpu.SemaphoreType.DMA((2,)),
                pltpu.SemaphoreType.DMA((2,)),
                pltpu.SemaphoreType.REGULAR,
            ],
            compiler_params=pltpu.CompilerParams(
                collective_id=0, has_side_effects=True, vmem_limit_bytes=37 * 2**20
            ),
            cost_estimate=pl.CostEstimate(
                flops=2 * rows * inner * cols, bytes_accessed=2**30, transcendentals=0
            ),
        )(a_rows, b_rows)
        held = [pltpu.with_memory_space_constraint(v, pltpu.VMEM) for v in outs[:3]]
        return pl.pallas_call(
            _close,
            out_shape=jax.ShapeDtypeStruct((rows, cols), bf16),
            in_specs=[vmem] * 3,
            out_specs=hbm,
            scratch_shapes=[
                pltpu.VMEM((2, rows, tn), bf16),
                pltpu.SemaphoreType.DMA((2, BANDS)),
                pltpu.SemaphoreType.DMA((2,)),
            ],
            compiler_params=pltpu.CompilerParams(vmem_limit_bytes=8 * 2**20),
        )(*held)

    return jax.shard_map(local_block, mesh=mesh, in_specs=(spec_rows, spec_rows), out_specs=spec_rows, check_vma=False)
```
